16 devices in a mesh: dp: 4 (over z, y), tp: 4 (over x, core).
Axes of the slice: x: 2, y: 2, z: 2, core: 2. Of those that a mesh axis runs over, the one named last changes fastest.
Arguments:
- hidden: bfloat16 [4, 2048, 1024], P('dp')
- norm_w: bfloat16 [1024], replicated
- embed_table: bfloat16 [151936, 1024], P('tp')
- labels: int32 [4, 2048], P('dp')
- loss_mask: int32 [4, 2048], P('dp')
Outputs:
- output 1: float32 [], replicated
- output 2: bfloat16 [4, 2048, 1024], P('dp')
- output 3: float32 [1024], replicated
- output 4: float32 [151936, 1024], P('tp')
All inputs are finite; a program needn't handle non-finite values.
Results may differ from the reference program's by a relative error of at most 0.001.
Values sent between devices are 32-bit elements.
A program may use at most 1 GiB of HBM per device.

```python
import math
import jax
import jax.numpy as jnp
from jax import lax

BATCH_ROWS = 4
SEQ_LEN = 2048
MODEL_DIM = 1024
VOCAB_SIZE = 151936
TOKEN_BLOCK = 128
SOFT_CAP = 30.0


def draw_labels(root_key):
    key_pick, key_common, key_any = jax.random.split(root_key, 3)
    label_shape = (BATCH_ROWS, SEQ_LEN)
    pick_val = jax.random.randint(key_pick, label_shape, 0, 4)
    common_id = jax.random.randint(key_common, label_shape, 0, VOCAB_SIZE // 32)
    any_id = jax.random.randint(key_any, label_shape, 0, VOCAB_SIZE)
    return jnp.where(pick_val == 0, any_id, common_id).astype(jnp.int32)


def draw_mask(root_key):
    key_rate, key_roll = jax.random.split(root_key, 2)
    drop_pct = jax.random.randint(key_rate, (BATCH_ROWS, 1), 5, 40)
    roll_val = jax.random.randint(key_roll, (BATCH_ROWS, SEQ_LEN), 0, 100)
    return (roll_val >= drop_pct).astype(jnp.int32)


def norm_apply(hid_rows, gain32):
    h32 = hid_rows.astype(jnp.float32)
    inv_rms = lax.rsqrt(jnp.mean(h32 * h32, axis=-1, keepdims=True) + 1e-6)
    return h32 * inv_rms * (1.0 + gain32)


def setup_inputs(seed: int = 0) -> dict:
    root_key = jax.random.key(seed)
    key_noise, key_gain, key_table, key_str, key_lab, key_mask, key_top = jax.random.split(root_key, 7)
    table_scale = 3.0 / math.sqrt(MODEL_DIM)
    table32 = jax.random.normal(key_table, (VOCAB_SIZE, MODEL_DIM), jnp.float32) * table_scale
    labels = draw_labels(key_lab)
    top_str = jax.random.uniform(key_top, (), jnp.float32, minval=3.0, maxval=6.5)
    strength = jax.random.uniform(key_str, (BATCH_ROWS, SEQ_LEN, 1), jnp.float32) * top_str
    noise_val = jax.random.normal(key_noise, (BATCH_ROWS, SEQ_LEN, MODEL_DIM), jnp.float32)
    hidden = noise_val + strength * jnp.take(table32, labels, axis=0)
    gain_vec = 0.3 * jax.random.normal(key_gain, (MODEL_DIM,), jnp.float32)
    return {'hidden': hidden.astype(jnp.bfloat16), 'norm_w': gain_vec.astype(jnp.bfloat16), 'embed_table': table32.astype(jnp.bfloat16), 'labels': labels, 'loss_mask': draw_mask(key_mask)}


def reference(hidden, norm_w, embed_table, labels, loss_mask):
    tokens = BATCH_ROWS * SEQ_LEN
    n_blocks = tokens // TOKEN_BLOCK
    hid_blocks = hidden.reshape(n_blocks, TOKEN_BLOCK, MODEL_DIM)
    lab_blocks = labels.reshape(n_blocks, TOKEN_BLOCK)
    mask_blocks = loss_mask.reshape(n_blocks, TOKEN_BLOCK).astype(jnp.float32)
    tok_count = jnp.maximum(jnp.sum(mask_blocks), 1.0)
    gain32 = norm_w.astype(jnp.float32)
    vocab_ids = jnp.arange(VOCAB_SIZE, dtype=jnp.int32)

    def block_step(carry_in, block_in):
        loss_sum, grad_gain, grad_table = carry_in
        hid_rows, lab_rows, mask_rows = block_in
        normed, norm_back = jax.vjp(norm_apply, hid_rows, gain32)
        normed_bf = normed.astype(jnp.bfloat16)
        logits = jnp.dot(normed_bf, embed_table.T, preferred_element_type=jnp.float32)
        capped = SOFT_CAP * jnp.tanh(logits / SOFT_CAP)
        row_max = jnp.max(capped, axis=-1, keepdims=True)
        exp_shift = jnp.exp(capped - row_max)
        row_sum = jnp.sum(exp_shift, axis=-1, keepdims=True)
        onehot = vocab_ids[None, :] == lab_rows[:, None]
        picked = jnp.sum(jnp.where(onehot, capped, 0.0), axis=-1)
        tok_loss = jnp.log(row_sum[:, 0]) + row_max[:, 0] - picked
        tok_scale = mask_rows / tok_count
        cap_ratio = capped / SOFT_CAP
        grad_logit = ((exp_shift / row_sum - onehot.astype(jnp.float32)) * tok_scale[:, None] * (1.0 - cap_ratio * cap_ratio)).astype(jnp.bfloat16)
        grad_x = jnp.dot(grad_logit, embed_table, preferred_element_type=jnp.float32)
        grad_rows, grad_g = norm_back(grad_x)
        table_part = jnp.dot(grad_logit.T, normed_bf, preferred_element_type=jnp.float32)
        new_carry = (loss_sum + jnp.sum(mask_rows * tok_loss), grad_gain + grad_g, grad_table + table_part)
        return new_carry, grad_rows

    init_carry = (jnp.zeros((), jnp.float32), jnp.zeros((MODEL_DIM,), jnp.float32), jnp.zeros((VOCAB_SIZE, MODEL_DIM), jnp.float32))
    final_carry, grad_rows = lax.scan(block_step, init_carry, (hid_blocks, lab_blocks, mask_blocks))
    loss_sum, grad_gain, grad_table = final_carry
    return loss_sum / tok_count, grad_rows.reshape(BATCH_ROWS, SEQ_LEN, MODEL_DIM), grad_gain, grad_table
```

```python
import functools
import math

import jax
import jax.numpy as jnp
from jax import lax
from jax.experimental import pallas as pl
from jax.experimental.pallas import tpu as pltpu
from jax.sharding import PartitionSpec as P

SOFT_CAP = 30.0
EXP2_CAP = 30.0 * math.log2(math.e)
VMEM_LIMIT = 67_000_000

CFG = dict(
    VB=1024,
    TS=512,
    RU=624,
    CHUNKS=(1, 3, 3, 2, 1),
    RD=592,
    CALLS=(6, 6, 6, 4),
    ABSORB=((0, 1), (), (2,), (3,)),
)
ANY = pl.BlockSpec(memory_space=pl.ANY)


def params(**kw):
    return pltpu.CompilerParams(vmem_limit_bytes=VMEM_LIMIT, **kw)


def dot_nt(a, b):
    return lax.dot_general(a, b, (((1,), (1,)), ((), ())), preferred_element_type=jnp.float32)


def first_pass(x, labels_rel, table):
    tokens, dim = x.shape
    rows = table.shape[0]
    vb, ts = CFG["VB"], CFG["TS"]
    n = pl.cdiv(rows, vb)
    last = rows - vb
    parts = tokens // ts

    def kernel(x_ref, lab_ref, e_ref, q_main, q_tail, z_sum, t_lab, z0, z1, carry, lab_b):
        s = pl.program_id(0)

        @pl.when(s == 0)
        def _():
            z_sum[...] = jnp.zeros_like(z_sum)
            t_lab[...] = jnp.zeros_like(t_lab)
            carry[...] = jnp.zeros_like(carry)
            lab_b[...] = jnp.broadcast_to(lab_ref[...], lab_b.shape)

        def elem(k, buf, blk, q_ref, q_row):
            start = jnp.minimum(blk * vb, last)
            ids = lax.broadcasted_iota(jnp.int32, (1, vb), 1) + start
            valid = jnp.logical_and(ids >= blk * vb, blk >= 0)
            bias = jnp.where(valid, 0.0, -1e30)
            ids = jnp.where(valid, ids, -1)
            for r in range(ts // 8):
                src = slice(r * 8, r * 8 + 8)
                row = slice(k * ts + r * 8, k * ts + r * 8 + 8)
                t = jnp.tanh(buf[src, :] * (1.0 / SOFT_CAP))
                e = jnp.exp2(t * EXP2_CAP + bias)
                q_ref[0, q_row + r * 8 : q_row + r * 8 + 8, :] = e * (1.0 - t * t)
                lab = lab_b[row, :]
                zs, tl = z_sum[row, :], t_lab[row, :]
                for c in range(vb // 128):
                    cs = slice(c * 128, (c + 1) * 128)
                    zs += e[:, cs]
                    tl += jnp.where(ids[:, cs] == lab, t[:, cs], 0.0)
                z_sum[row, :] = zs
                t_lab[row, :] = tl

        def dot(k, buf):
            buf[...] = dot_nt(x_ref[k * ts : (k + 1) * ts, :], e_ref[...])

        def tail():
            elem(parts - 1, carry, s - 1, q_tail, 0)

        @pl.when(s < n)
        def _():
            bufs = [(z0, z1)[k % 2] for k in range(parts - 1)] + [carry]
            dot(0, bufs[0])
            tail()
            for k in range(1, parts):
                dot(k, bufs[k])
                elem(k - 1, bufs[k - 1], s, q_main, (k - 1) * ts)

        @pl.when(s == n)
        def _():
            tail()

    col = pl.BlockSpec((tokens, 128), lambda s: (0, 0))
    return pl.pallas_call(
        kernel,
        grid=(n + 1,),
        in_specs=[
            pl.BlockSpec((tokens, dim), lambda s: (0, 0), pipeline_mode=pl.Buffered(1)),
            pl.BlockSpec((tokens, 1), lambda s: (0, 0), pipeline_mode=pl.Buffered(1)),
            pl.BlockSpec((pl.Element(vb), pl.Element(dim)), lambda s: (jnp.minimum(s * (vb // 16), last // 16) * 16, 0)),
        ],
        out_specs=[
            pl.BlockSpec((1, tokens - ts, vb), lambda s: (jnp.minimum(s, n - 1), 0, 0)),
            pl.BlockSpec((1, ts, vb), lambda s: (jnp.maximum(s - 1, 0), 0, 0)),
            col,
            col,
        ],
        out_shape=[
            jax.ShapeDtypeStruct((n, tokens - ts, vb), jnp.float32),
            jax.ShapeDtypeStruct((n, ts, vb), jnp.float32),
            jax.ShapeDtypeStruct((tokens, 128), jnp.float32),
            jax.ShapeDtypeStruct((tokens, 128), jnp.float32),
        ],
        scratch_shapes=[pltpu.VMEM((ts, vb), jnp.float32)] * 3 + [pltpu.VMEM((tokens, 128), jnp.int32)],
        compiler_params=params(dimension_semantics=("arbitrary",)),
        cost_estimate=pl.CostEstimate(flops=2 * tokens * rows * dim, bytes_accessed=tokens * rows * 4, transcendentals=0),
        name="first_pass",
    )(x, labels_rel, table)


def grad_x(q_main, q_tail, table, a_col, b_col, labels_rel, dep):
    n, ts, vb = q_tail.shape
    tokens = q_main.shape[1] + ts
    rows, dim = table.shape
    last = rows - vb

    def kernel(qm_ref, qt_ref, e_ref, a_ref, b_ref, lab_ref, dep_ref, gx_ref, a_b, b_b, lab_b, *g_bufs):
        s = pl.program_id(0)

        @pl.when(s == 0)
        def _():
            gx_ref[...] = jnp.zeros_like(gx_ref)
            a_b[...] = jnp.broadcast_to(a_ref[...], a_b.shape)
            b_b[...] = jnp.broadcast_to(b_ref[...], b_b.shape)
            lab_b[...] = jnp.broadcast_to(lab_ref[...], lab_b.shape)

        start = jnp.minimum(s * vb, last)
        ids = lax.broadcasted_iota(jnp.int32, (1, vb), 1) + start
        ids = jnp.where(ids >= s * vb, ids, -1)
        for k in range(tokens // ts):
            g_buf = g_bufs[k % 2]
            q_ref, row = (qm_ref, k * ts) if k < tokens // ts - 1 else (qt_ref, 0)
            for r in range(ts // 16):
                sl = slice(k * ts + r * 16, k * ts + r * 16 + 16)
                a, b, lab = a_b[sl, :], b_b[sl, :], lab_b[sl, :]
                for c in range(vb // 128):
                    cs = slice(c * 128, (c + 1) * 128)
                    g = q_ref[0, row + r * 16 : row + r * 16 + 16, cs] * a - jnp.where(ids[:, cs] == lab, b, 0.0)
                    g_buf[r * 16 : r * 16 + 16, cs] = g.astype(jnp.bfloat16)
            gx_ref[k * ts : (k + 1) * ts, :] += jnp.dot(g_buf[...], e_ref[...], preferred_element_type=jnp.float32)

    col = pl.BlockSpec((tokens, 1), lambda s: (0, 0), pipeline_mode=pl.Buffered(1))
    return pl.pallas_call(
        kernel,
        grid=(n,),
        in_specs=[
            pl.BlockSpec((1, tokens - ts, vb), lambda s: (s, 0, 0)),
            pl.BlockSpec((1, ts, vb), lambda s: (s, 0, 0)),
            pl.BlockSpec((pl.Element(vb), pl.Element(dim)), lambda s: (jnp.minimum(s * (vb // 16), last // 16) * 16, 0)),
            col,
            col,
            col,
            ANY,
        ],
        out_specs=pl.BlockSpec((tokens, dim), lambda s: (0, 0)),
        out_shape=jax.ShapeDtypeStruct((tokens, dim), jnp.float32),
        scratch_shapes=[
            pltpu.VMEM((tokens, 128), jnp.float32),
            pltpu.VMEM((tokens, 128), jnp.float32),
            pltpu.VMEM((tokens, 128), jnp.int32),
            pltpu.VMEM((ts, vb), jnp.bfloat16),
            pltpu.VMEM((ts, vb), jnp.bfloat16),
        ],
        compiler_params=params(dimension_semantics=("arbitrary",)),
        cost_estimate=pl.CostEstimate(flops=2 * tokens * rows * dim, bytes_accessed=tokens * rows * 4, transcendentals=0),
        name="grad_x",
    )(q_main, q_tail, table, a_col, b_col, labels_rel, dep)


def table_rows(offset, table, x_all, lab, inv_z, scale, rb, nblk, dep, out=None, out_base=0, out_rows=None, sources=()):
    dim = table.shape[1]
    ntc, _, ts = lab.shape
    tokens = ntc * ts
    in_half = ntc // 2
    pieces = []
    for k, (src, row) in enumerate(sources):
        m = CFG["RU"]
        pieces += [(k, p * m, row + p * m) for p in range(src.shape[0] // m)]
    per_block = ntc // 2 - 1
    assert not pieces or len(pieces) + 2 <= nblk * per_block
    rows_total = out.shape[0] if out is not None else out_rows

    def kernel(off_ref, e_hbm, x_a, x_b, lab_ref, iz_ref, sc_ref, dep_ref, *rest):
        rest, x_hbm = list(rest), (x_a, x_b)
        srcs = [rest.pop(0) for _ in sources]
        if out is not None:
            rest.pop(0)
        o_hbm = rest.pop(0)
        xv, ebuf, z0, z1, g0, g1, acc, xsem, esem, osem = rest[:10]
        if pieces:
            pbuf, lsem, ssem = rest[10:]
        zs, gs = (z0, z1), (g0, g1)
        i = pl.program_id(0)
        slot = lax.rem(i, 2)
        off = off_ref[0]

        def x_copy(j):
            src = x_hbm[j // in_half] if isinstance(j, int) else x_hbm[0]
            row = j % in_half if isinstance(j, int) else 0
            dst = pl.ds(pl.multiple_of(j * ts, ts), ts)
            return pltpu.make_async_copy(src.at[pl.ds(row * ts, ts), :], xv.at[dst, :], xsem.at[j])

        def e_copy(b, sl):
            return pltpu.make_async_copy(e_hbm.at[pl.ds(pl.multiple_of(off + b * rb, 16), rb), :], ebuf.at[sl], esem.at[sl])

        def o_copy(b, sl):
            return pltpu.make_async_copy(acc.at[sl], o_hbm.at[pl.ds(pl.multiple_of(out_base + b * rb, 8), rb), :], osem.at[sl])

        @pl.when(i == 0)
        def _():
            e_copy(0, 0).start()
            for j in range(ntc):
                x_copy(j).start()

        @pl.when(i + 1 < nblk)
        def _():
            e_copy(i + 1, 1 - slot).start()

        e_copy(i, slot).wait()

        @pl.when(i >= 2)
        def _():
            o_copy(i - 2, slot).wait()

        def wait_x(*js):
            @pl.when(i == 0)
            def _():
                for j in js:
                    x_copy(j).wait()

        def xs(j):
            return xv[pl.ds(pl.multiple_of(j * ts, ts), ts), :]

        def dot1(j, p):
            zs[p][...] = dot_nt(ebuf[slot], xs(j))

        def elem(j, p):
            rel = lab_ref[j] - (off + i * rb)
            iz, sc = iz_ref[j], sc_ref[j]
            for r in range(rb // 16):
                sl = slice(r * 16, r * 16 + 16)
                t = jnp.tanh(zs[p][sl, :] * (1.0 / SOFT_CAP))
                e = jnp.exp2(t * EXP2_CAP) * iz
                ids = lax.broadcasted_iota(jnp.int32, (16, ts), 0) + r * 16
                d = jnp.where(ids == rel, e - 1.0, e)
                gs[p][sl, :] = (d * sc * (1.0 - t * t)).astype(jnp.bfloat16)

        def dot2(j, p):
            acc[slot] += jnp.dot(gs[p][...], xs(j), preferred_element_type=jnp.float32)

        def piece_step(it):
            if not pieces:
                return
            for idx, (k, a, b) in enumerate(pieces):
                m = CFG["RU"]
                load = pltpu.make_async_copy(srcs[k].at[a : a + m, :], pbuf.at[idx % 2], lsem.at[idx % 2])
                store = pltpu.make_async_copy(pbuf.at[idx % 2], o_hbm.at[b : b + m, :], ssem.at[idx % 2])

                @pl.when(it == idx)
                def _():
                    if idx >= 2:
                        pltpu.make_async_copy(pbuf.at[idx % 2], o_hbm.at[0:m, :], ssem.at[idx % 2]).wait()
                    load.start()

                @pl.when(it == idx + 1)
                def _():
                    load.wait()
                    store.start()

        acc[slot] = jnp.zeros(acc.shape[1:], acc.dtype)
        wait_x(0, 1)
        dot1(0, 0)
        elem(0, 0)
        dot1(1, 1)

        def body(jj, c):
            j = 2 * jj
            wait_x(j, j + 1)
            piece_step(i * per_block + jj - 1)
            dot2(j - 2, 0)
            elem(j - 1, 1)
            dot1(j, 0)
            dot2(j - 1, 1)
            elem(j, 0)
            dot1(j + 1, 1)
            return c

        lax.fori_loop(1, ntc // 2, body, 0)
        dot2(ntc - 2, 0)
        elem(ntc - 1, 1)
        dot2(ntc - 1, 1)
        o_copy(i, slot).start()

        @pl.when(i == nblk - 1)
        def _():
            o_copy(i, slot).wait()
            if nblk >= 2:
                o_copy(i - 1, 1 - slot).wait()
            if pieces:
                for idx in range(max(0, len(pieces) - 2), len(pieces)):
                    m = CFG["RU"]
                    pltpu.make_async_copy(pbuf.at[idx % 2], o_hbm.at[0:m, :], ssem.at[idx % 2]).wait()

    vec = pl.BlockSpec((ntc, 1, ts), lambda i: (0, 0, 0), pipeline_mode=pl.Buffered(1))
    scratch = [
        pltpu.VMEM((tokens, dim), jnp.bfloat16),
        pltpu.VMEM((2, rb, dim), jnp.bfloat16),
        pltpu.VMEM((rb, ts), jnp.float32),
        pltpu.VMEM((rb, ts), jnp.float32),
        pltpu.VMEM((rb, ts), jnp.bfloat16),
        pltpu.VMEM((rb, ts), jnp.bfloat16),
        pltpu.VMEM((2, rb, dim), jnp.float32),
        pltpu.SemaphoreType.DMA((ntc,)),
        pltpu.SemaphoreType.DMA((2,)),
        pltpu.SemaphoreType.DMA((2,)),
    ]
    if pieces:
        scratch += [pltpu.VMEM((2, CFG["RU"], dim), jnp.float32), pltpu.SemaphoreType.DMA((2,)), pltpu.SemaphoreType.DMA((2,))]
    args = [offset, table, *x_all, lab, inv_z, scale, dep] + [s for s, _ in sources] + ([out] if out is not None else [])
    return pl.pallas_call(
        kernel,
        grid=(nblk,),
        in_specs=[pl.BlockSpec(memory_space=pltpu.SMEM), ANY, ANY, ANY, vec, vec, vec, ANY] + [ANY] * (len(args) - 8),
        out_specs=ANY,
        out_shape=jax.ShapeDtypeStruct((rows_total, dim), jnp.float32),
        scratch_shapes=scratch,
        input_output_aliases={len(args) - 1: 0} if out is not None else {},
        compiler_params=params(dimension_semantics=("arbitrary",)),
        cost_estimate=pl.CostEstimate(flops=4 * tokens * rb * nblk * dim, bytes_accessed=tokens * dim * 2, transcendentals=0),
        name="table_rows",
    )(*args)


def place(out, src, row):
    rows, dim = src.shape
    m = rows // 4

    def kernel(src_ref, o_in, o_ref, buf, lsem, ssem):
        loads = [pltpu.make_async_copy(src_ref.at[k * m : (k + 1) * m, :], buf.at[k], lsem.at[k]) for k in range(4)]
        stores = [pltpu.make_async_copy(buf.at[k], o_ref.at[row + k * m : row + (k + 1) * m, :], ssem.at[k]) for k in range(4)]
        for c in loads:
            c.start()
        for a, b in zip(loads, stores):
            a.wait()
            b.start()
        for c in stores:
            c.wait()

    return pl.pallas_call(
        kernel,
        in_specs=[ANY, ANY],
        out_specs=ANY,
        out_shape=jax.ShapeDtypeStruct(out.shape, out.dtype),
        scratch_shapes=[pltpu.VMEM((4, m, dim), jnp.float32), pltpu.SemaphoreType.DMA((4,)), pltpu.SemaphoreType.DMA((4,))],
        input_output_aliases={1: 0},
        compiler_params=params(),
        cost_estimate=pl.CostEstimate(flops=rows * dim, bytes_accessed=rows * dim * 8, transcendentals=0),
        name="place",
    )(src, out)


def norm_apply(hid_rows, gain32):
    h32 = hid_rows.astype(jnp.float32)
    inv_rms = lax.rsqrt(jnp.mean(h32 * h32, axis=-1, keepdims=True) + 1e-6)
    return h32 * inv_rms * (1.0 + gain32)


def solution(mesh):
    n_dp, n_tp = mesh.shape["dp"], mesh.shape["tp"]
    sib = [(i, i ^ 1) for i in range(n_tp)]
    across = [(i, i ^ 2) for i in range(n_tp)]

    def local_step(hidden, norm_w, table, labels, loss_mask):
        batch, seq, dim = hidden.shape
        rows = table.shape[0]
        tokens = batch * seq
        half = tokens // 2
        ts = CFG["TS"]
        dp, tp = lax.axis_index("dp"), lax.axis_index("tp")
        core = lax.rem(tp, 2)
        hid = hidden.reshape(tokens, dim)
        normed, norm_back = jax.vjp(norm_apply, hid, norm_w.astype(jnp.float32))
        x = normed.astype(jnp.bfloat16)
        lab_own = labels.reshape(tokens)
        lab_rel = (lab_own - tp * rows)[:, None]

        def mine(v):
            return jnp.where(core == 0, v[:half], v[half:])

        hid32 = hid.astype(jnp.float32)
        pre = mine(hid32 * lax.rsqrt(jnp.mean(hid32 * hid32, axis=-1, keepdims=True) + 1e-6))
        got = lax.all_gather(pre, "dp", axis=0, tiled=True)

        q_main, q_tail, z_sum, t_lab = first_pass(x, lab_rel, table)
        got, z_sum = lax.optimization_barrier((got, z_sum))
        other = lax.ppermute(got, "tp", sib)
        gain = 1.0 + norm_w.astype(jnp.float32)
        x_all = tuple((v * gain).astype(jnp.bfloat16) for v in (got, other))
        side = jnp.stack([lab_own, loss_mask.reshape(tokens)]).astype(jnp.float32)
        stats = jnp.stack([jnp.sum(z_sum, axis=-1), jnp.sum(t_lab, axis=-1)])
        stats = jnp.concatenate([stats, jnp.where(tp == 0, side, 0.0)])
        stats = lax.dynamic_update_slice(jnp.zeros((n_dp, 4, tokens), jnp.float32), stats[None], (dp, 0, 0))
        stats = lax.psum(stats, ("dp", "tp"))

        split = stats.reshape(n_dp, 4, 2, half)
        split = jnp.where(core == 0, split, split[:, :, ::-1])
        z_all, t_all, lab_all, mask_all = split.transpose(1, 2, 0, 3).reshape(4, -1)
        lab_all = lab_all.astype(jnp.int32)
        count = jnp.maximum(jnp.sum(mask_all), 1.0)
        loss = jnp.sum(mask_all * (jnp.log(z_all) - SOFT_CAP * t_all)) / count
        scale_all = mask_all / count
        shape3 = (n_dp * tokens // ts, 1, ts)
        vecs = ((lab_all - tp * rows).reshape(shape3), (1.0 / z_all).reshape(shape3), scale_all.reshape(shape3))

        own = lax.dynamic_index_in_dim(stats, dp, 0, keepdims=False)
        scale_own = loss_mask.reshape(tokens).astype(jnp.float32) / count
        a_col = (scale_own / own[0])[:, None]
        b_col = (scale_own * (1.0 - own[1] * own[1]))[:, None]

        ru, rd = CFG["RU"], CFG["RD"]
        dep, row, gathered = x, 0, []
        for nblk in CFG["CHUNKS"]:
            off = (row + dp * (nblk * ru)).astype(jnp.int32).reshape(1)
            dep = table_rows(off, table, x_all, *vecs, ru, nblk, dep, out_rows=nblk * ru)
            gathered.append((lax.all_gather(dep, "dp", axis=0, tiled=True), row))
            row += n_dp * nblk * ru

        gx = grad_x(q_main, q_tail, table, a_col, b_col, lab_rel, dep)
        keep = jnp.where(core == 0, gx[:half], gx[half:])
        send = jnp.where(core == 0, gx[half:], gx[:half])
        out = None
        for k, (nblk, absorb) in enumerate(zip(CFG["CALLS"], CFG["ABSORB"])):
            off = jnp.full((1,), row, jnp.int32)
            src = tuple(gathered[c] for c in absorb)
            if k < 3:
                recv = lax.ppermute(send, "tp", (sib, across, sib)[k])
            out = table_rows(off, table, x_all, *vecs, rd, nblk, send, out=out, out_base=row, out_rows=rows, sources=src)
            row += nblk * rd
            if k < 3:
                recv, out = lax.optimization_barrier((recv, out))
            if k < 2:
                send = keep = keep + recv
        gx_all = jnp.where(core == 0, jnp.concatenate([keep, recv]), jnp.concatenate([recv, keep]))
        grad_rows, grad_gain = norm_back(gx_all)
        grad_gain = lax.psum(grad_gain, "dp")
        assert row == rows
        out = place(out, *gathered[-1])
        return loss, grad_rows.reshape(batch, seq, dim), grad_gain, out

    return jax.shard_map(
        local_step,
        mesh=mesh,
        in_specs=(P("dp", None, None), P(None), P("tp", None), P("dp", None), P("dp", None)),
        out_specs=(P(), P("dp", None, None), P(None), P("tp", None)),
        check_vma=False,
    )
```

```python
import functools
import math

import jax
import jax.numpy as jnp
from jax import lax
from jax.experimental import pallas as pl
from jax.experimental.pallas import tpu as pltpu
from jax.sharding import PartitionSpec as P

SOFT_CAP = 30.0
EXP2_CAP = 30.0 * math.log2(math.e)
VMEM_LIMIT = 67_000_000

CFG = dict(
    VB=1024,
    TS=512,
    RU=720,
    CHUNKS=(1, 3, 3, 2, 1),
    RD=656,
    CALLS=(4, 4, 3, 3),
    ABSORB=((0, 1), (), (2,), (3,)),
)
ANY = pl.BlockSpec(memory_space=pl.ANY)


def params(**kw):
    return pltpu.CompilerParams(vmem_limit_bytes=VMEM_LIMIT, **kw)


def dot_nt(a, b):
    return lax.dot_general(a, b, (((1,), (1,)), ((), ())), preferred_element_type=jnp.float32)


def first_pass(x, labels_rel, table):
    tokens, dim = x.shape
    rows = table.shape[0]
    vb, ts = CFG["VB"], CFG["TS"]
    n = pl.cdiv(rows, vb)
    last = rows - vb
    parts = tokens // ts

    def kernel(x_ref, lab_ref, e_ref, q_main, q_tail, z_sum, t_lab, z0, z1, carry, lab_b):
        s = pl.program_id(0)

        @pl.when(s == 0)
        def _():
            z_sum[...] = jnp.zeros_like(z_sum)
            t_lab[...] = jnp.zeros_like(t_lab)
            carry[...] = jnp.zeros_like(carry)
            lab_b[...] = jnp.broadcast_to(lab_ref[...], lab_b.shape)

        def elem(k, buf, blk, q_ref, q_row):
            start = jnp.minimum(blk * vb, last)
            ids = lax.broadcasted_iota(jnp.int32, (1, vb), 1) + start
            valid = jnp.logical_and(ids >= blk * vb, blk >= 0)
            bias = jnp.where(valid, 0.0, -1e30)
            ids = jnp.where(valid, ids, -1)
            for r in range(ts // 8):
                src = slice(r * 8, r * 8 + 8)
                row = slice(k * ts + r * 8, k * ts + r * 8 + 8)
                t = jnp.tanh(buf[src, :] * (1.0 / SOFT_CAP))
                e = jnp.exp2(t * EXP2_CAP + bias)
                q_ref[0, q_row + r * 8 : q_row + r * 8 + 8, :] = e * (1.0 - t * t)
                lab = lab_b[row, :]
                zs, tl = z_sum[row, :], t_lab[row, :]
                for c in range(vb // 128):
                    cs = slice(c * 128, (c + 1) * 128)
                    zs += e[:, cs]
                    tl += jnp.where(ids[:, cs] == lab, t[:, cs], 0.0)
                z_sum[row, :] = zs
                t_lab[row, :] = tl

        def dot(k, buf):
            buf[...] = dot_nt(x_ref[k * ts : (k + 1) * ts, :], e_ref[...])

        def tail():
            elem(parts - 1, carry, s - 1, q_tail, 0)

        @pl.when(s < n)
        def _():
            bufs = [(z0, z1)[k % 2] for k in range(parts - 1)] + [carry]
            dot(0, bufs[0])
            tail()
            for k in range(1, parts):
                dot(k, bufs[k])
                elem(k - 1, bufs[k - 1], s, q_main, (k - 1) * ts)

        @pl.when(s == n)
        def _():
            tail()

    col = pl.BlockSpec((tokens, 128), lambda s: (0, 0))
    return pl.pallas_call(
        kernel,
        grid=(n + 1,),
        in_specs=[
            pl.BlockSpec((tokens, dim), lambda s: (0, 0), pipeline_mode=pl.Buffered(1)),
            pl.BlockSpec((tokens, 1), lambda s: (0, 0), pipeline_mode=pl.Buffered(1)),
            pl.BlockSpec((pl.Element(vb), pl.Element(dim)), lambda s: (jnp.minimum(s * (vb // 16), last // 16) * 16, 0)),
        ],
        out_specs=[
            pl.BlockSpec((1, tokens - ts, vb), lambda s: (jnp.minimum(s, n - 1), 0, 0)),
            pl.BlockSpec((1, ts, vb), lambda s: (jnp.maximum(s - 1, 0), 0, 0)),
            col,
            col,
        ],
        out_shape=[
            jax.ShapeDtypeStruct((n, tokens - ts, vb), jnp.float32),
            jax.ShapeDtypeStruct((n, ts, vb), jnp.float32),
            jax.ShapeDtypeStruct((tokens, 128), jnp.float32),
            jax.ShapeDtypeStruct((tokens, 128), jnp.float32),
        ],
        scratch_shapes=[pltpu.VMEM((ts, vb), jnp.float32)] * 3 + [pltpu.VMEM((tokens, 128), jnp.int32)],
        compiler_params=params(dimension_semantics=("arbitrary",)),
        cost_estimate=pl.CostEstimate(flops=2 * tokens * rows * dim, bytes_accessed=tokens * rows * 4, transcendentals=0),
        name="first_pass",
    )(x, labels_rel, table)


def grad_x(q_main, q_tail, table, a_col, b_col, labels_rel, dep):
    n, ts, vb = q_tail.shape
    tokens = q_main.shape[1] + ts
    rows, dim = table.shape
    last = rows - vb

    def kernel(qm_ref, qt_ref, e_ref, a_ref, b_ref, lab_ref, dep_ref, gx_ref, a_b, b_b, lab_b, *g_bufs):
        s = pl.program_id(0)

        @pl.when(s == 0)
        def _():
            gx_ref[...] = jnp.zeros_like(gx_ref)
            a_b[...] = jnp.broadcast_to(a_ref[...], a_b.shape)
            b_b[...] = jnp.broadcast_to(b_ref[...], b_b.shape)
            lab_b[...] = jnp.broadcast_to(lab_ref[...], lab_b.shape)

        start = jnp.minimum(s * vb, last)
        ids = lax.broadcasted_iota(jnp.int32, (1, vb), 1) + start
        ids = jnp.where(ids >= s * vb, ids, -1)
        for k in range(tokens // ts):
            g_buf = g_bufs[k % 2]
            q_ref, row = (qm_ref, k * ts) if k < tokens // ts - 1 else (qt_ref, 0)
            for r in range(ts // 16):
                sl = slice(k * ts + r * 16, k * ts + r * 16 + 16)
                a, b, lab = a_b[sl, :], b_b[sl, :], lab_b[sl, :]
                for c in range(vb // 128):
                    cs = slice(c * 128, (c + 1) * 128)
                    g = q_ref[0, row + r * 16 : row + r * 16 + 16, cs] * a - jnp.where(ids[:, cs] == lab, b, 0.0)
                    g_buf[r * 16 : r * 16 + 16, cs] = g.astype(jnp.bfloat16)
            gx_ref[k * ts : (k + 1) * ts, :] += jnp.dot(g_buf[...], e_ref[...], preferred_element_type=jnp.float32)

    col = pl.BlockSpec((tokens, 1), lambda s: (0, 0), pipeline_mode=pl.Buffered(1))
    return pl.pallas_call(
        kernel,
        grid=(n,),
        in_specs=[
            pl.BlockSpec((1, tokens - ts, vb), lambda s: (s, 0, 0)),
            pl.BlockSpec((1, ts, vb), lambda s: (s, 0, 0)),
            pl.BlockSpec((pl.Element(vb), pl.Element(dim)), lambda s: (jnp.minimum(s * (vb // 16), last // 16) * 16, 0)),
            col,
            col,
            col,
            ANY,
        ],
        out_specs=pl.BlockSpec((tokens, dim), lambda s: (0, 0)),
        out_shape=jax.ShapeDtypeStruct((tokens, dim), jnp.float32),
        scratch_shapes=[
            pltpu.VMEM((tokens, 128), jnp.float32),
            pltpu.VMEM((tokens, 128), jnp.float32),
            pltpu.VMEM((tokens, 128), jnp.int32),
            pltpu.VMEM((ts, vb), jnp.bfloat16),
            pltpu.VMEM((ts, vb), jnp.bfloat16),
        ],
        compiler_params=params(dimension_semantics=("arbitrary",)),
        cost_estimate=pl.CostEstimate(flops=2 * tokens * rows * dim, bytes_accessed=tokens * rows * 4, transcendentals=0),
        name="grad_x",
    )(q_main, q_tail, table, a_col, b_col, labels_rel, dep)


def table_rows(offset, table, x_all, lab, inv_z, scale, rb, nblk, dep, out=None, out_base=0, out_rows=None, sources=()):
    dim = table.shape[1]
    ntc, _, ts = lab.shape
    tokens = ntc * ts
    in_half = ntc // 2
    pieces = []
    for k, (src, row) in enumerate(sources):
        m = CFG["RU"]
        pieces += [(k, p * m, row + p * m) for p in range(src.shape[0] // m)]
    per_block = ntc // 2 - 1
    assert not pieces or len(pieces) + 2 <= nblk * per_block
    rows_total = out.shape[0] if out is not None else out_rows

    def kernel(off_ref, e_hbm, x_a, x_b, lab_ref, iz_ref, sc_ref, dep_ref, *rest):
        rest, x_hbm = list(rest), (x_a, x_b)
        srcs = [rest.pop(0) for _ in sources]
        if out is not None:
            rest.pop(0)
        o_hbm = rest.pop(0)
        xv, ebuf, z0, z1, g0, g1, acc, xsem, esem, osem = rest[:10]
        if pieces:
            pbuf, lsem, ssem = rest[10:]
        zs, gs = (z0, z1), (g0, g1)
        i = pl.program_id(0)
        slot = lax.rem(i, 2)
        off = off_ref[0]

        def x_copy(j):
            src = x_hbm[j // in_half] if isinstance(j, int) else x_hbm[0]
            row = j % in_half if isinstance(j, int) else 0
            dst = pl.ds(pl.multiple_of(j * ts, ts), ts)
            return pltpu.make_async_copy(src.at[pl.ds(row * ts, ts), :], xv.at[dst, :], xsem.at[j])

        def e_copy(b, sl):
            return pltpu.make_async_copy(e_hbm.at[pl.ds(pl.multiple_of(off + b * rb, 16), rb), :], ebuf.at[sl], esem.at[sl])

        def o_copy(b, sl):
            return pltpu.make_async_copy(acc.at[sl], o_hbm.at[pl.ds(pl.multiple_of(out_base + b * rb, 8), rb), :], osem.at[sl])

        @pl.when(i == 0)
        def _():
            e_copy(0, 0).start()
            for j in range(ntc):
                x_copy(j).start()

        @pl.when(i + 1 < nblk)
        def _():
            e_copy(i + 1, 1 - slot).start()

        e_copy(i, slot).wait()

        @pl.when(i >= 2)
        def _():
            o_copy(i - 2, slot).wait()

        def wait_x(*js):
            @pl.when(i == 0)
            def _():
                for j in js:
                    x_copy(j).wait()

        def xs(j):
            return xv[pl.ds(pl.multiple_of(j * ts, ts), ts), :]

        def dot1(j, p):
            zs[p][...] = dot_nt(ebuf[slot], xs(j))

        def elem(j, p):
            rel = lab_ref[j] - (off + i * rb)
            iz, sc = iz_ref[j], sc_ref[j]
            for r in range(rb // 16):
                sl = slice(r * 16, r * 16 + 16)
                t = jnp.tanh(zs[p][sl, :] * (1.0 / SOFT_CAP))
                e = jnp.exp2(t * EXP2_CAP) * iz
                ids = lax.broadcasted_iota(jnp.int32, (16, ts), 0) + r * 16
                d = jnp.where(ids == rel, e - 1.0, e)
                gs[p][sl, :] = (d * sc * (1.0 - t * t)).astype(jnp.bfloat16)

        def dot2(j, p):
            acc[slot] += jnp.dot(gs[p][...], xs(j), preferred_element_type=jnp.float32)

        def piece_step(it):
            if not pieces:
                return
            for idx, (k, a, b) in enumerate(pieces):
                m = CFG["RU"]
                load = pltpu.make_async_copy(srcs[k].at[a : a + m, :], pbuf.at[idx % 2], lsem.at[idx % 2])
                store = pltpu.make_async_copy(pbuf.at[idx % 2], o_hbm.at[b : b + m, :], ssem.at[idx % 2])

                @pl.when(it == idx)
                def _():
                    if idx >= 2:
                        pltpu.make_async_copy(pbuf.at[idx % 2], o_hbm.at[0:m, :], ssem.at[idx % 2]).wait()
                    load.start()

                @pl.when(it == idx + 1)
                def _():
                    load.wait()
                    store.start()

        acc[slot] = jnp.zeros(acc.shape[1:], acc.dtype)
        wait_x(0, 1)
        dot1(0, 0)
        elem(0, 0)
        dot1(1, 1)

        def body(jj, c):
            j = 2 * jj
            wait_x(j, j + 1)
            piece_step(i * per_block + jj - 1)
            dot2(j - 2, 0)
            elem(j - 1, 1)
            dot1(j, 0)
            dot2(j - 1, 1)
            elem(j, 0)
            dot1(j + 1, 1)
            return c

        lax.fori_loop(1, ntc // 2, body, 0)
        dot2(ntc - 2, 0)
        elem(ntc - 1, 1)
        dot2(ntc - 1, 1)
        o_copy(i, slot).start()

        @pl.when(i == nblk - 1)
        def _():
            o_copy(i, slot).wait()
            if nblk >= 2:
                o_copy(i - 1, 1 - slot).wait()
            if pieces:
                for idx in range(max(0, len(pieces) - 2), len(pieces)):
                    m = CFG["RU"]
                    pltpu.make_async_copy(pbuf.at[idx % 2], o_hbm.at[0:m, :], ssem.at[idx % 2]).wait()

    vec = pl.BlockSpec((ntc, 1, ts), lambda i: (0, 0, 0), pipeline_mode=pl.Buffered(1))
    scratch = [
        pltpu.VMEM((tokens, dim), jnp.bfloat16),
        pltpu.VMEM((2, rb, dim), jnp.bfloat16),
        pltpu.VMEM((rb, ts), jnp.float32),
        pltpu.VMEM((rb, ts), jnp.float32),
        pltpu.VMEM((rb, ts), jnp.bfloat16),
        pltpu.VMEM((rb, ts), jnp.bfloat16),
        pltpu.VMEM((2, rb, dim), jnp.float32),
        pltpu.SemaphoreType.DMA((ntc,)),
        pltpu.SemaphoreType.DMA((2,)),
        pltpu.SemaphoreType.DMA((2,)),
    ]
    if pieces:
        scratch += [pltpu.VMEM((2, CFG["RU"], dim), jnp.float32), pltpu.SemaphoreType.DMA((2,)), pltpu.SemaphoreType.DMA((2,))]
    args = [offset, table, *x_all, lab, inv_z, scale, dep] + [s for s, _ in sources] + ([out] if out is not None else [])
    return pl.pallas_call(
        kernel,
        grid=(nblk,),
        in_specs=[pl.BlockSpec(memory_space=pltpu.SMEM), ANY, ANY, ANY, vec, vec, vec, ANY] + [ANY] * (len(args) - 8),
        out_specs=ANY,
        out_shape=jax.ShapeDtypeStruct((rows_total, dim), jnp.float32),
        scratch_shapes=scratch,
        input_output_aliases={len(args) - 1: 0} if out is not None else {},
        compiler_params=params(dimension_semantics=("arbitrary",)),
        cost_estimate=pl.CostEstimate(flops=4 * tokens * rb * nblk * dim, bytes_accessed=tokens * dim * 2, transcendentals=0),
        name="table_rows",
    )(*args)


def place(out, src, row):
    rows, dim = src.shape
    m = rows // 4

    def kernel(src_ref, o_in, o_ref, buf, lsem, ssem):
        loads = [pltpu.make_async_copy(src_ref.at[k * m : (k + 1) * m, :], buf.at[k], lsem.at[k]) for k in range(4)]
        stores = [pltpu.make_async_copy(buf.at[k], o_ref.at[row + k * m : row + (k + 1) * m, :], ssem.at[k]) for k in range(4)]
        for c in loads:
            c.start()
        for a, b in zip(loads, stores):
            a.wait()
            b.start()
        for c in stores:
            c.wait()

    return pl.pallas_call(
        kernel,
        in_specs=[ANY, ANY],
        out_specs=ANY,
        out_shape=jax.ShapeDtypeStruct(out.shape, out.dtype),
        scratch_shapes=[pltpu.VMEM((4, m, dim), jnp.float32), pltpu.SemaphoreType.DMA((4,)), pltpu.SemaphoreType.DMA((4,))],
        input_output_aliases={1: 0},
        compiler_params=params(),
        cost_estimate=pl.CostEstimate(flops=rows * dim, bytes_accessed=rows * dim * 8, transcendentals=0),
        name="place",
    )(src, out)


def norm_apply(hid_rows, gain32):
    h32 = hid_rows.astype(jnp.float32)
    inv_rms = lax.rsqrt(jnp.mean(h32 * h32, axis=-1, keepdims=True) + 1e-6)
    return h32 * inv_rms * (1.0 + gain32)


def solution(mesh):
    n_dp, n_tp = mesh.shape["dp"], mesh.shape["tp"]
    sib = [(i, i ^ 1) for i in range(n_tp)]
    across = [(i, i ^ 2) for i in range(n_tp)]

    def local_step(hidden, norm_w, table, labels, loss_mask):
        batch, seq, dim = hidden.shape
        rows = table.shape[0]
        tokens = batch * seq
        half = tokens // 2
        ts = CFG["TS"]
        dp, tp = lax.axis_index("dp"), lax.axis_index("tp")
        core = lax.rem(tp, 2)
        hid = hidden.reshape(tokens, dim)
        normed, norm_back = jax.vjp(norm_apply, hid, norm_w.astype(jnp.float32))
        x = normed.astype(jnp.bfloat16)
        lab_own = labels.reshape(tokens)
        lab_rel = (lab_own - tp * rows)[:, None]

        def mine(v):
            return jnp.where(core == 0, v[:half], v[half:])

        hid32 = hid.astype(jnp.float32)
        pre = mine(hid32 * lax.rsqrt(jnp.mean(hid32 * hid32, axis=-1, keepdims=True) + 1e-6))
        got = lax.all_gather(pre, "dp", axis=0, tiled=True)

        q_main, q_tail, z_sum, t_lab = first_pass(x, lab_rel, table)
        got, z_sum = lax.optimization_barrier((got, z_sum))
        other = lax.ppermute(got, "tp", sib)
        gain = 1.0 + norm_w.astype(jnp.float32)
        x_all = tuple((v * gain).astype(jnp.bfloat16) for v in (got, other))
        side = jnp.stack([lab_own, loss_mask.reshape(tokens)]).astype(jnp.float32)
        stats = jnp.stack([jnp.sum(z_sum, axis=-1), jnp.sum(t_lab, axis=-1)])
        own = lax.psum(stats, "tp")
        stats = lax.all_gather(jnp.concatenate([own, side]), "dp", axis=0, tiled=False)

        split = stats.reshape(n_dp, 4, 2, half)
        split = jnp.where(core == 0, split, split[:, :, ::-1])
        z_all, t_all, lab_all, mask_all = split.transpose(1, 2, 0, 3).reshape(4, -1)
        lab_all = lab_all.astype(jnp.int32)
        count = jnp.maximum(jnp.sum(mask_all), 1.0)
        loss = jnp.sum(mask_all * (jnp.log(z_all) - SOFT_CAP * t_all)) / count
        scale_all = mask_all / count
        shape3 = (n_dp * tokens // ts, 1, ts)
        vecs = ((lab_all - tp * rows).reshape(shape3), (1.0 / z_all).reshape(shape3), scale_all.reshape(shape3))

        scale_own = loss_mask.reshape(tokens).astype(jnp.float32) / count
        a_col = (scale_own / own[0])[:, None]
        b_col = (scale_own * (1.0 - own[1] * own[1]))[:, None]

        ru, rd = CFG["RU"], CFG["RD"]
        dep, row, gathered = x, 0, []
        for nblk in CFG["CHUNKS"]:
            off = (row + dp * (nblk * ru)).astype(jnp.int32).reshape(1)
            dep = table_rows(off, table, x_all, *vecs, ru, nblk, dep, out_rows=nblk * ru)
            gathered.append((lax.all_gather(dep, "dp", axis=0, tiled=True), row))
            row += n_dp * nblk * ru

        gx = grad_x(q_main, q_tail, table, a_col, b_col, lab_rel, dep)
        keep = jnp.where(core == 0, gx[:half], gx[half:])
        send = jnp.where(core == 0, gx[half:], gx[:half])
        out = None
        for k, (nblk, absorb) in enumerate(zip(CFG["CALLS"], CFG["ABSORB"])):
            off = jnp.full((1,), row, jnp.int32)
            src = tuple(gathered[c] for c in absorb)
            if k < 3:
                recv = lax.ppermute(send, "tp", (sib, across, sib)[k])
            out = table_rows(off, table, x_all, *vecs, rd, nblk, send, out=out, out_base=row, out_rows=rows, sources=src)
            row += nblk * rd
            if k < 3:
                recv, out = lax.optimization_barrier((recv, out))
            if k < 2:
                send = keep = keep + recv
        gx_all = jnp.where(core == 0, jnp.concatenate([keep, recv]), jnp.concatenate([recv, keep]))
        grad_rows, grad_gain = norm_back(gx_all)
        grad_gain = lax.psum(grad_gain, "dp")
        assert row == rows
        out = place(out, *gathered[-1])
        return loss, grad_rows.reshape(batch, seq, dim), grad_gain, out

    return jax.shard_map(
        local_step,
        mesh=mesh,
        in_specs=(P("dp", None, None), P(None), P("tp", None), P("dp", None), P("dp", None)),
        out_specs=(P(), P("dp", None, None), P(None), P("tp", None)),
        check_vma=False,
    )
```
